32 devices in a mesh: shard: 8 (over z, y), tp: 4 (over x, core).
Axes of the slice: x: 2, y: 2, z: 4, core: 2. Of those that a mesh axis runs over, the one named last changes fastest.
Arguments:
- weight_query: bfloat16 [12288, 12288], P('shard', 'tp'), may hold values from -0.078125 to 0.078125
- low_query: bfloat16 [12288, 64], P('shard'), may hold values from -0.0546875 to 0.0546875
- high_query: bfloat16 [64, 12288], P(None, 'tp'), may hold values from -0.75 to 0.75
- weight_key: bfloat16 [12288, 12288], P('shard', 'tp'), may hold values from -0.078125 to 0.078125
- low_key: bfloat16 [12288, 64], P('shard'), may hold values from -0.0546875 to 0.0546875
- high_key: bfloat16 [64, 12288], P(None, 'tp'), may hold values from -0.75 to 0.75
- weight_value: bfloat16 [12288, 12288], P('shard', 'tp'), may hold values from -0.078125 to 0.078125
- low_value: bfloat16 [12288, 64], P('shard'), may hold values from -0.0546875 to 0.0546875
- high_value: bfloat16 [64, 12288], P(None, 'tp'), may hold values from -0.75 to 0.75
- norm_train: float32 [12288], P(('shard', 'tp')), may hold values from 0.25 to 1.75
- norm_step: float32 [12288], P(('shard', 'tp')), may hold values from -0.3 to 0.3
Outputs:
- ready_query: bfloat16 [12288, 12288], P(None, ('tp', 'shard'))
- ready_key: bfloat16 [12288, 12288], P(None, ('tp', 'shard'))
- ready_value: bfloat16 [12288, 12288], P(None, ('tp', 'shard'))
- column_query: float32 [12288], P(('tp', 'shard'))
- column_key: float32 [12288], P(('tp', 'shard'))
- column_value: float32 [12288], P(('tp', 'shard'))
- serve_norm: bfloat16 [12288], replicated
The draws below stay inside these ranges and needn't reach their ends.
All inputs are finite; a program needn't handle non-finite values. Where the reference program divides by a largest or mean magnitude, that divisor is 1e-20 or more.
Results may differ from the reference program's by a relative error of at most 0.001.
Values may be sent and summed in bfloat16 or wider, within the bound.
A program may use at most 192 MiB of HBM per device.

```python
import jax
import jax.numpy as jnp

D_MODEL = 12288
Q_DIM = 12288
KV_DIM = 12288
RANK = 64


def with_spikes(values, key, source, target, parts, factor):
    owner, partner = [(jnp.arange(values.shape[position]) // (values.shape[position] // parts)).reshape([-1 if axis == position else 1 for axis in range(values.ndim)]) for position in (source, target)]
    chosen = jax.random.permutation(key, parts)[partner]
    strong = (owner == chosen) | (owner == (partner + parts // 2) % parts)
    return jnp.where(strong, factor * values, values)


def levels(stream_key, dims, shards, smallest, largest):
    loudness = 1.0
    for dim, parts in shards:
        draws = jax.random.uniform(jax.random.fold_in(jax.random.fold_in(stream_key, 6), dim), (parts,), jnp.float32, smallest / len(shards), largest / len(shards))
        loudness = loudness * jnp.repeat(jnp.exp(draws), dims[dim] // parts).reshape((-1,) + (1,) * (len(dims) - 1 - dim))
    return loudness


def bell_draw(key, extent, spread, bound, cuts=(), kind=jnp.bfloat16):
    loudness = levels(key, extent, cuts, -0.22, 0.18) if cuts else 1.0
    values = jax.random.normal(key, extent, jnp.float32) * spread * loudness
    return jnp.minimum(jnp.maximum(values, -bound), bound).astype(kind)


def heavy_noise(key, extent, width, most, shards, heavy, kind=jnp.bfloat16):
    array = width * jax.random.normal(key, extent, jnp.float32)
    if shards:
        array = array * levels(key, extent, shards, -0.22, 0.18)
    return jnp.clip(with_spikes(array, jax.random.fold_in(key, 3), *heavy), -most, most).astype(kind)


def setup_inputs(seed: int = 0) -> dict:
    seeds = jax.random.split(jax.random.key(seed), 12)
    return {
        "weight_query": heavy_noise(seeds[0], (D_MODEL, Q_DIM), D_MODEL ** -0.5, 0.078125, ((0, 8), (1, 4)), (0, 1, 8, 2.0)),
        "low_query": bell_draw(seeds[1], (D_MODEL, RANK), D_MODEL ** -0.5, 0.0546875, ((0, 8),)),
        "high_query": bell_draw(seeds[2], (RANK, Q_DIM), RANK ** -0.5, 0.75, ((1, 4),)),
        "weight_key": heavy_noise(seeds[3], (D_MODEL, KV_DIM), D_MODEL ** -0.5, 0.078125, ((0, 8), (1, 4)), (0, 1, 8, 2.0)),
        "low_key": bell_draw(seeds[4], (D_MODEL, RANK), D_MODEL ** -0.5, 0.0546875, ((0, 8),)),
        "high_key": bell_draw(seeds[5], (RANK, KV_DIM), RANK ** -0.5, 0.75, ((1, 4),)),
        "weight_value": heavy_noise(seeds[6], (D_MODEL, KV_DIM), D_MODEL ** -0.5, 0.078125, ((0, 8), (1, 4)), (0, 1, 8, 2.0)),
        "low_value": bell_draw(seeds[7], (D_MODEL, RANK), D_MODEL ** -0.5, 0.0546875, ((0, 8),)),
        "high_value": bell_draw(seeds[8], (RANK, KV_DIM), RANK ** -0.5, 0.75, ((1, 4),)),
        "norm_train": jnp.clip(1.0 + 0.15 * jax.random.normal(seeds[9], (D_MODEL,), jnp.float32), 0.25, 1.75),
        "norm_step": jnp.clip(jax.random.uniform(seeds[10], (D_MODEL,), jnp.float32, -0.3, 0.3) * levels(seeds[10], (D_MODEL,), ((0, 32),), -0.4, 0.0), -0.3, 0.3),
    }


mix_rate = 0.5


def reference(weight_query, low_query, high_query, weight_key, low_key, high_key, weight_value, low_value, high_value, norm_train, norm_step):
    latest_query = weight_query.astype(jnp.float32) + mix_rate * jnp.dot(low_query, high_query, preferred_element_type=jnp.float32)
    latest_key = weight_key.astype(jnp.float32) + mix_rate * jnp.dot(low_key, high_key, preferred_element_type=jnp.float32)
    latest_value = weight_value.astype(jnp.float32) + mix_rate * jnp.dot(low_value, high_value, preferred_element_type=jnp.float32)
    column_query = jnp.sum(jnp.abs(latest_query), axis=0) / D_MODEL
    ready_query = (latest_query / column_query).astype(jnp.bfloat16)
    column_key = jnp.sum(jnp.abs(latest_key), axis=0) / D_MODEL
    ready_key = (latest_key / column_key).astype(jnp.bfloat16)
    column_value = jnp.sum(jnp.abs(latest_value), axis=0) / D_MODEL
    ready_value = (latest_value / column_value).astype(jnp.bfloat16)
    serve_norm = (norm_train + norm_step).astype(jnp.bfloat16)
    return ready_query, ready_key, ready_value, column_query, column_key, column_value, serve_norm
```

```python
import functools

import jax
import jax.numpy as jnp
from jax import lax
from jax.experimental import pallas as pl
from jax.experimental.pallas import tpu as pltpu
from jax.sharding import PartitionSpec as P

mix_rate = 0.5
MESH = pl.DeviceIdType.MESH
TILE = 256
RAW = 128


def merged(weight, low, high):
    product = jnp.dot(low, high, preferred_element_type=jnp.float32)
    return weight.astype(jnp.float32) + mix_rate * product


def exchange(
    n, parts, depth,
    wq, wk, wv, lq, lk, lv, hq, hk, hv, train, step,
    land_q, land_k, land_v, col_out, norm_out,
    wbuf, ltbuf, lbuf, hbuf, stat, col, raw, rawlow, fin, norm,
    load_sem, high_sem, low_sem, own_sem, fin_sem,
    send_sem, recv_sem, stat_send, stat_recv, raw_send, raw_recv,
    rlow_send, rlow_recv, norm_send, norm_recv, side_send, side_recv,
):
    weights, lows, highs = (wq, wk, wv), (lq, lk, lv), (hq, hk, hv)
    lands = (land_q, land_k, land_v)
    rows, width = wbuf.shape[2], wbuf.shape[3]
    me, side = lax.axis_index("shard"), lax.axis_index("tp")
    half = n // 2
    top, low_place = me // half, me % half

    def target(k):
        return lax.rem(1 - top + k // half, 2) * half + lax.rem(low_place + k % half, half)

    def cols(k):
        return pl.ds(pl.multiple_of(target(k) * width, 128), width)

    order = list(range(n))
    others = [k for k in order if k != half]
    loads = {}
    for m in range(3):
        low_copy = pltpu.make_async_copy(lows[m], ltbuf.at[m], low_sem.at[m])
        low_copy.start()
        loads[m] = low_copy
        for k in order:
            loads[m, k] = (
                pltpu.make_async_copy(highs[m].at[:, cols(k)], hbuf.at[m, k], high_sem.at[m, k]),
                pltpu.make_async_copy(weights[m].at[:, cols(k)], wbuf.at[m, k], load_sem.at[m, k]),
            )
            for copy in loads[m, k]:
                copy.start()

    norm[side, me, 0, :] = train[...] + step[...]

    barrier = pltpu.get_barrier_semaphore()
    for k in others:
        pl.semaphore_signal(barrier, inc=1, device_id={"shard": target(k)}, device_id_type=MESH)
    for j in range(1, parts):
        pl.semaphore_signal(
            barrier, inc=1, device_id={"tp": lax.rem(side + j, parts)}, device_id_type=MESH
        )
    pl.semaphore_wait(barrier, n - 1 + parts - 1)

    def remote(src, dst, send, recv, device):
        copy = pltpu.make_async_remote_copy(
            src_ref=src, dst_ref=dst, send_sem=send, recv_sem=recv,
            device_id=device, device_id_type=MESH,
        )
        copy.start()
        return copy

    raws, raw_lows = [], []
    for k in range(half):
        there = {"shard": target(k)}
        raw_lows.append(remote(
            lv.at[:, pl.ds(0, RAW)], rawlow.at[k], rlow_send.at[k], rlow_recv.at[k], there
        ))
        raws.append(remote(
            wv.at[pl.ds(0, RAW), cols(k)], raw.at[k], raw_send.at[k], raw_recv.at[k], there
        ))
    norms = [
        remote(norm.at[side, me], norm.at[side, me], norm_send.at[k], norm_recv.at[k], {"shard": target(k)})
        for k in others
    ]

    def sums(m):
        loads[m].wait()
        lbuf[m] = jnp.transpose(ltbuf[m].astype(jnp.float32)).astype(jnp.bfloat16)
        for k in order:
            for copy in loads[m, k]:
                copy.wait()

            def tile(i, total):
                at = pl.ds(pl.multiple_of(i * TILE, TILE), TILE)
                latest = merged(wbuf[m, k, at, :], lbuf[m, at, :], hbuf[m, k])
                return total + jnp.sum(jnp.abs(latest), axis=0, keepdims=True)

            total = lax.fori_loop(0, rows // TILE, tile, jnp.zeros((1, width), jnp.float32))
            stat[m, me, pl.ds(target(k), 1), :] = total
        return [
            remote(stat.at[m, me], stat.at[m, me], stat_send.at[m, k], stat_recv.at[m, k], {"shard": target(k)})
            for k in others
        ]

    def columns(m, copies):
        for copy in copies:
            copy.wait()
        total = stat[m, 0]
        for s in range(1, n):
            total = total + stat[m, s]
        col[m] = total / depth
        col_out[m] = col[m, pl.ds(me, 1), :]

    sent, own = [], []

    def send(m, k):
        first = RAW if m == 2 and k < half else 0
        if k == half:
            copy = pltpu.make_async_copy(
                wbuf.at[m, k], lands[m].at[pl.ds(pl.multiple_of(me * rows, 16), rows)], own_sem.at[m]
            )
            copy.start()
            own.append(copy)
            return
        sent.append(remote(
            wbuf.at[m, k, pl.ds(first, rows - first)],
            lands[m].at[pl.ds(pl.multiple_of(me * rows + first, 16), rows - first)],
            send_sem.at[m, k], recv_sem.at[m, k], {"shard": target(k)},
        ))

    def ready(m, behind):
        for k in order:
            scale = col[m, pl.ds(target(k), 1), :]

            def tile(i, carry):
                at = pl.ds(pl.multiple_of(i * TILE, TILE), TILE)
                latest = merged(wbuf[m, k, at, :], lbuf[m, at, :], hbuf[m, k])
                wbuf[m, k, at, :] = (latest / scale).astype(jnp.bfloat16)
                return carry

            lax.fori_loop(0, rows // TILE, tile, 0)
            if behind is not None:
                send(*behind)
            behind = (m, k)
        return behind

    stats = [sums(0), sums(1)]
    columns(0, stats[0])
    behind = ready(0, None)
    stats.append(sums(2))
    columns(1, stats[1])
    behind = ready(1, behind)
    columns(2, stats[2])
    behind = ready(2, behind)
    send(*behind)

    for copy in norms:
        copy.wait()
    sides = [
        remote(norm.at[side], norm.at[side], side_send.at[j], side_recv.at[j], {"tp": lax.rem(side + j, parts)})
        for j in range(1, parts)
    ]

    scale = col[2, pl.ds(me, 1), :]
    fins = []
    for k in range(half):
        raw_lows[k].wait()
        raws[k].wait()
        low = jnp.transpose(rawlow[k].astype(jnp.float32)).astype(jnp.bfloat16)
        latest = merged(raw[k], low, hbuf[2, half])
        fin[k] = (latest / scale).astype(jnp.bfloat16)
        source = (1 - top) * half + lax.rem(low_place + half - k, half)
        copy = pltpu.make_async_copy(
            fin.at[k], land_v.at[pl.ds(pl.multiple_of(source * rows, 16), RAW)], fin_sem.at[k]
        )
        copy.start()
        fins.append(copy)

    for copy in sides:
        copy.wait()
    norm_out[...] = norm[...]
    for copy in fins + own + sent:
        copy.wait()


def copy_out(q_in, k_in, v_in, q_out, k_out, v_out):
    q_out[...] = q_in[...]
    k_out[...] = k_in[...]
    v_out[...] = v_in[...]


def kernel_body(
    n, parts,
    weight_query, low_query, high_query,
    weight_key, low_key, high_key,
    weight_value, low_value, high_value,
    norm_train, norm_step,
):
    rows, wide = weight_query.shape
    width, depth = wide // n, rows * n
    rank, piece = low_query.shape[1], norm_train.shape[0]
    anywhere = pl.BlockSpec(memory_space=pl.ANY)
    vmem = pl.BlockSpec(memory_space=pltpu.VMEM)
    land = jax.ShapeDtypeStruct((depth, width), jnp.bfloat16)
    dma = pltpu.SemaphoreType.DMA
    half = n // 2
    land_q, land_k, land_v, column, norm = pl.pallas_call(
        functools.partial(exchange, n, parts, depth),
        out_shape=(
            land, land, land,
            jax.ShapeDtypeStruct((3, 1, width), jnp.float32),
            jax.ShapeDtypeStruct((parts, n, 1, piece), jnp.float32),
        ),
        in_specs=[anywhere] * 9 + [vmem] * 2,
        out_specs=(anywhere, anywhere, anywhere, vmem, vmem),
        scratch_shapes=[
            pltpu.VMEM((3, n, rows, width), jnp.bfloat16),
            pltpu.VMEM((3, rank, rows), jnp.bfloat16),
            pltpu.VMEM((3, rows, rank), jnp.bfloat16),
            pltpu.VMEM((3, n, rank, width), jnp.bfloat16),
            pltpu.VMEM((3, n, n, width), jnp.float32),
            pltpu.VMEM((3, n, width), jnp.float32),
            pltpu.VMEM((half, RAW, width), jnp.bfloat16),
            pltpu.VMEM((half, rank, RAW), jnp.bfloat16),
            pltpu.VMEM((half, RAW, width), jnp.bfloat16),
            pltpu.VMEM((parts, n, 1, piece), jnp.float32),
            dma((3, n)), dma((3, n)), dma((3,)), dma((3,)), dma((half,)),
            dma((3, n)), dma((3, n)), dma((3, n)), dma((3, n)),
            dma((half,)), dma((half,)), dma((half,)), dma((half,)),
            dma((n,)), dma((n,)), dma((parts,)), dma((parts,)),
        ],
        compiler_params=pltpu.CompilerParams(
            collective_id=0, has_side_effects=True, vmem_limit_bytes=56 * 2**20
        ),
        name="exchange",
    )(
        weight_query, weight_key, weight_value,
        low_query.T, low_key.T, low_value.T,
        high_query, high_key, high_value,
        norm_train, norm_step,
    )
    steps = 8
    block = pl.BlockSpec((depth // steps, width), lambda i: (i, 0))
    outs = pl.pallas_call(
        copy_out,
        grid=(steps,),
        out_shape=(land, land, land),
        in_specs=[block] * 3,
        out_specs=(block,) * 3,
        compiler_params=pltpu.CompilerParams(vmem_limit_bytes=48 * 2**20),
        name="copy_out",
    )(land_q, land_k, land_v)
    serve = jnp.transpose(norm.reshape(parts, n, piece), (1, 0, 2)).reshape(-1)
    return (*outs, column[0, 0], column[1, 0], column[2, 0], serve.astype(jnp.bfloat16))


def plain_body(
    weight_query, low_query, high_query,
    weight_key, low_key, high_key,
    weight_value, low_value, high_value,
    norm_train, norm_step,
):
    n = lax.axis_size("shard")
    latest = [
        merged(weight, low, high)
        for weight, low, high in (
            (weight_query, low_query, high_query),
            (weight_key, low_key, high_key),
            (weight_value, low_value, high_value),
        )
    ]
    totals = lax.psum(tuple(jnp.sum(jnp.abs(x), axis=0) for x in latest), "shard")
    place = lax.axis_index("shard")
    readies, columns = [], []
    for x, total in zip(latest, totals):
        column = total / (x.shape[0] * n)
        narrow = (x / column).astype(jnp.bfloat16)
        ready = lax.all_to_all(narrow, "shard", split_axis=1, concat_axis=0, tiled=True)
        readies.append(ready)
        columns.append(lax.dynamic_slice_in_dim(column, place * ready.shape[1], ready.shape[1]))
    serve = (norm_train + norm_step).astype(jnp.bfloat16)
    serve = lax.all_gather(serve, ("shard", "tp"), tiled=True)
    return (*readies, *columns, serve)


def solution(mesh):
    n, parts = mesh.shape["shard"], mesh.shape["tp"]

    def body(*args):
        rows, wide = args[0].shape
        fits = (
            n % 2 == 0
            and wide % (n * 128) == 0
            and rows % TILE == 0
            and all(args[i].shape == args[0].shape for i in (3, 6))
            and 6 * rows * wide < 40 * 2**20
        )
        if fits:
            return kernel_body(n, parts, *args)
        return plain_body(*args)

    weight, low, high = P("shard", "tp"), P("shard", None), P(None, "tp")
    norm = P(("shard", "tp"))
    ready, column = P(None, ("tp", "shard")), P(("tp", "shard"))
    return jax.shard_map(
        body,
        mesh=mesh,
        in_specs=(weight, low, high) * 3 + (norm, norm),
        out_specs=(ready,) * 3 + (column,) * 3 + (P(),),
        check_vma=False,
    )
```
